256 devices in a mesh: dp: 32 (over x, z_lo, core), sub: 8 (over z_hi, y).
Axes of the slice: x: 4, y: 4, z: 8 (z_hi: 2, z_lo: 4; z = z_hi * 4 + z_lo), core: 2. Of those that a mesh axis runs over, the one named last changes fastest.
Arguments:
- context: bfloat16 [403456, 1024], P(('dp', 'sub')), may hold values from -6 to 6
- target: bfloat16 [403456, 1024], P(('dp', 'sub')), may hold values from -16 to 16
- weight: float32 [1024, 1024], P(('dp', 'sub')), may hold values from -0.1875 to 0.1875
- stale: bfloat16 [256, 1024, 1024], P(('dp', 'sub')), may hold values from -1.25 to 1.25
- trigger: int32 [256, 16], P(('dp', 'sub')), may hold values 0 or 1
- aggregate: float32 [1024, 1024], P(('dp', 'sub')), may hold values from -3 to 3
- moment: float32 [1024, 1024], P(('dp', 'sub')), may hold values from -0.6 to 0.6
- second: float32 [1024, 1024], P(('dp', 'sub')), may hold values from 0.0001 to 0.01
Outputs:
- aggregate_new: float32 [1024, 1024], P(('dp', 'sub'))
- weight_new: float32 [1024, 1024], P(('dp', 'sub'))
- moment_new: float32 [1024, 1024], P(('dp', 'sub'))
- second_new: float32 [1024, 1024], P(('dp', 'sub'))
- stale_new: bfloat16 [256, 1024, 1024], P(('dp', 'sub'))
- norms: float32 [16], replicated
The draws below stay inside these ranges and needn't reach their ends.
All inputs are finite; a program needn't handle non-finite values. No bound on the sum of `trigger` on one device may be relied on, other than what follows from the above.
Results may differ from the reference program's by a relative error of at most 0.006.
Values may be sent and summed in bfloat16 or wider, within the bound.
A program may use at most 64 MiB of HBM per device.

```python
import math
import jax
import jax.numpy as jnp
from jax import lax

D = 1024
BLOCKS = 16
ROWS = 1576
TOKENS = 403456
N_DP = 32
N_SUB = 8


def draw_target(key, part):
    rows = jnp.arange(TOKENS, dtype=jnp.float32)
    rising = 1.0 + 2.0 * rows / TOKENS
    base = jax.random.truncated_normal(key, -4.0, 4.0, (TOKENS, D), jnp.float32)
    values = base * rising[:, None]
    return values.astype(jnp.bfloat16)


def touch_ends(entries, stream_key, low, high):
    dims = entries.shape
    index_at = [jax.random.randint(jax.random.fold_in(stream_key, axis), (), 0, dims[axis]) for axis in range(len(dims))]
    entries = entries.at[tuple(index_at)].set(low)
    longest = dims.index(max(dims))
    index_at[longest] = (index_at[longest] + 1) % dims[longest]
    return entries.at[tuple(index_at)].set(high)


def raised(entries, own_key, source, target, parts, factor):
    owner, partner = [(jnp.arange(entries.shape[position]) // (entries.shape[position] // parts)).reshape([-1 if axis == position else 1 for axis in range(entries.ndim)]) for position in (source, target)]
    chosen = jax.random.permutation(own_key, parts)[partner]
    strong = (owner == chosen) | (owner == (partner + parts // 2) % parts)
    return jnp.where(strong, factor * entries, entries)


def shard_levels(stream_key, dims, shards, smallest, high):
    level, own = 1.0, jax.random.fold_in(stream_key, 6)
    for position, parts in shards:
        steps = jnp.exp(jax.random.uniform(jax.random.fold_in(own, position), (parts,), jnp.float32, smallest / len(shards), high / len(shards)))
        level = level * jnp.repeat(steps, dims[position] // parts).reshape([-1 if axis == position else 1 for axis in range(len(dims))])
    return level


def gaussian(own_key, dims, spread, most, cuts=(), kind=jnp.bfloat16):
    values = jax.random.normal(own_key, dims, jnp.float32) * spread
    if len(cuts) > 0:
        values = shard_levels(own_key, dims, cuts, -0.22, 0.18) * values
    return jnp.clip(values, min=-most, max=most).astype(kind)


def noise_with(key, shape, width, reach, shards, heavy, kind=jnp.bfloat16):
    drawn = width * jax.random.normal(key, shape, jnp.float32)
    if shards:
        drawn = drawn * shard_levels(key, shape, shards, -0.22, 0.18)
    return jnp.clip(raised(drawn, jax.random.fold_in(key, 3), *heavy), -reach, reach).astype(kind)


def setup_inputs(seed: int = 0) -> dict:
    splits = jax.random.split(jax.random.key(seed), 9)
    return {
        "context": gaussian(splits[0], (TOKENS, D), 1.0, 6.0, ((0, 256),)),
        "target": draw_target(jax.random.fold_in(splits[8], 71), 0),
        "weight": gaussian(splits[2], (D, D), D ** -0.5, 0.1875, ((0, 256),), jnp.float32),
        "stale": noise_with(splits[3], (N_DP * N_SUB, D, D), 0.05, 1.25, ((0, 256),), (0, 1, 256, 6.0)),
        "trigger": touch_ends((jax.random.randint(splits[4], (N_DP * N_SUB, BLOCKS), 0, 2) < 1).astype(jnp.int32), jax.random.fold_in(splits[4], 1), 0, 1),
        "aggregate": gaussian(splits[5], (D, D), 0.5, 3.0, ((0, 256),), jnp.float32),
        "moment": gaussian(splits[6], (D, D), 0.1, 0.6, ((0, 256),), jnp.float32),
        "second": jnp.clip(jnp.exp(math.log(0.01) - 4.6051702 * jax.random.uniform(splits[7], (D, D), jnp.float32) ** shard_levels(splits[7], (D, D), ((0, 256),), -0.2, 0.2)), 0.0001, 0.01),
    }


def reference(context, target, weight, stale, trigger, aggregate, moment, second):
    devices = N_DP * N_SUB
    low = weight.astype(jnp.bfloat16)
    span = D // BLOCKS

    def one(carry, index):
        total, squares = carry
        rows_ctx = lax.dynamic_slice_in_dim(context, index * ROWS, ROWS, 0)
        rows_tgt = lax.dynamic_slice_in_dim(target, index * ROWS, ROWS, 0)
        output = jnp.dot(rows_ctx, low, preferred_element_type=jnp.float32)
        error = (output - rows_tgt.astype(jnp.float32)).astype(jnp.bfloat16)
        grad = lax.dot_general(rows_ctx, error, (((0,), (0,)), ((), ())), preferred_element_type=jnp.float32) / ROWS
        old = lax.dynamic_index_in_dim(stale, index, 0, keepdims=False).astype(jnp.float32)
        flags = lax.dynamic_index_in_dim(trigger, index, 0, keepdims=False).astype(jnp.float32)
        diff = grad - old
        blocked = diff.reshape(BLOCKS, span, D)
        squares = squares + lax.optimization_barrier(jnp.sum(blocked * blocked, axis=(1, 2)))
        chosen = (blocked * flags[:, None, None]).reshape(D, D)
        fresh = (flags[:, None, None] * grad.reshape(BLOCKS, span, D) + (1.0 - flags[:, None, None]) * old.reshape(BLOCKS, span, D)).reshape(D, D)
        return ((total + chosen, squares), fresh.astype(jnp.bfloat16))
    start = (jnp.zeros((D, D), jnp.float32), jnp.zeros((BLOCKS,), jnp.float32))
    (total, norms), stale_new = lax.scan(one, start, jnp.arange(devices, dtype=jnp.int32))
    aggregate_new = aggregate + total
    moment_new = 0.9 * moment + 0.1 * aggregate_new
    second_new = 0.999 * second + 0.001 * aggregate_new * aggregate_new
    weight_new = weight - 0.001 * (moment_new / (jnp.sqrt(second_new) + 1e-08) + 0.05 * weight)
    return (aggregate_new, weight_new, moment_new, second_new, stale_new, norms)
```

```python
import functools

import jax
import jax.numpy as jnp
from jax import lax
from jax.experimental import pallas as pl
from jax.experimental.pallas import tpu as pltpu
from jax.sharding import PartitionSpec as P

MESH = pl.DeviceIdType.MESH
F32 = jnp.float32
BF16 = jnp.bfloat16
CHUNKS = 4
NX = 4
NY = 4
NZ = 8
PIECE = 4


def step_kernel(
    rows,
    padded,
    context,
    target,
    weight,
    stale,
    trigger,
    summed_out,
    stale_out,
    norms_out,
    cbuf,
    ct,
    tbuf,
    sbuf,
    fbuf,
    perm,
    perm_t,
    wz,
    wz32,
    wbuf,
    wn,
    ebuf,
    half,
    drecv,
    asend,
    arecv,
    bsend,
    brecv,
    zsend,
    zrecv,
    sqacc,
    nrm,
    nx_buf,
    ny_buf,
    nz_buf,
    cin_sem,
    tin_sem,
    sin_sem,
    fout_sem,
    gz_s,
    gz_r,
    gb_s,
    gb_r,
    ga_s,
    ga_r,
    gd_s,
    gd_r,
    rd_s,
    rd_r,
    ra_s,
    ra_r,
    rb_s,
    rb_r,
    rz_s,
    rz_r,
    n_s,
    n_r,
):
    width = context.shape[1]
    cols = width // CHUNKS
    dp = lax.axis_index("dp")
    sub = lax.axis_index("sub")
    c = lax.rem(dp, 2)
    x = lax.div(dp, 8)
    zlo = lax.rem(lax.div(dp, 2), 4)
    zhi = lax.div(sub, NY)
    y = lax.rem(sub, NY)
    z = zhi * 4 + zlo
    am = x * (1 - c) + y * c
    bm = y * (1 - c) + x * c

    def device(px, py, pz, pc):
        return ((px * 4 + lax.rem(pz, 4)) * 2 + pc, lax.div(pz, 4) * NY + py)

    def a_peer(a):
        return device(a * (1 - c) + x * c, y * (1 - c) + a * c, z, c)

    def b_peer(b):
        return device(x * (1 - c) + b * c, b * (1 - c) + y * c, z, c)

    def x_peer(k):
        return device(lax.rem(x + k, NX), y, z, c)

    def y_peer(k):
        return device(x, lax.rem(y + k, NY), z, c)

    def z_peer(k):
        return device(x, y, lax.rem(z + k, NZ), c)

    partner = device(x, y, z, 1 - c)

    def remote(src, dst, s, r, to):
        return pltpu.make_async_remote_copy(
            src_ref=src, dst_ref=dst, send_sem=s, recv_sem=r, device_id=to, device_id_type=MESH
        )

    context_in = pltpu.make_async_copy(context, cbuf.at[pl.ds(0, rows)], cin_sem)
    context_in.start()
    target_in = []
    stale_in = []
    for j in range(CHUNKS):
        part = pl.ds(j * cols, cols)
        target_in.append(
            pltpu.make_async_copy(target.at[:, part], tbuf.at[j, pl.ds(0, rows)], tin_sem.at[j])
        )
        stale_in.append(pltpu.make_async_copy(stale.at[0, :, part], sbuf.at[j], sin_sem.at[j]))
        target_in[j].start()
        stale_in[j].start()

    barrier = pltpu.get_barrier_semaphore()
    greeted = [partner]
    greeted += [x_peer(k) for k in range(1, NX)]
    greeted += [y_peer(k) for k in range(1, NY)]
    greeted += [z_peer(k) for k in range(1, NZ)]
    for to in greeted:
        pl.semaphore_signal(barrier, inc=1, device_id=to, device_id_type=MESH)

    group = 2 * NY * NZ * PIECE
    place = lax.broadcasted_iota(jnp.int32, (group, group), 0)
    natural = lax.broadcasted_iota(jnp.int32, (group, group), 1)

    def natural_of(i):
        ic, iy, iz, ir = i // 128, (i // 32) % 4, (i // 4) % 8, i % 4
        return (iz % 4) * 64 + ic * 32 + (iz // 4) * 16 + iy * 4 + ir

    perm[...] = jnp.where(natural == natural_of(place), 1.0, 0.0).astype(BF16)
    perm_t[...] = jnp.where(place == natural_of(natural), 1.0, 0.0).astype(BF16)
    tail = padded - rows
    cbuf[pl.ds(rows, tail)] = jnp.zeros((tail, width), BF16)
    ebuf[...] = jnp.zeros((padded, cols), BF16)
    for j in range(CHUNKS):
        tbuf[j, pl.ds(rows, tail)] = jnp.zeros((tail, cols), BF16)
    sqacc[...] = jnp.zeros(sqacc.shape, F32)

    pl.semaphore_wait(barrier, len(greeted))

    gz = []
    for k in range(1, NZ):
        gz.append(remote(weight, wz.at[z], gz_s.at[k - 1], gz_r.at[k - 1], z_peer(k)))
        gz[-1].start()
    wz[z] = weight[...]
    context_in.wait()

    def turn(m, carry):
        span = pl.ds(pl.multiple_of(m * 128, 128), 128)
        ct[:, span] = cbuf[span, :].T
        return carry

    blocks = padded // 128
    lax.fori_loop(0, 6, turn, 0)
    for copy in gz:
        copy.wait_recv()
    for i in range(NZ):
        wz32[pl.ds(i * PIECE, PIECE), :] = wz[i]
    own = wz32[...].astype(BF16)
    gb = []
    for j in range(CHUNKS):
        wbuf[j, c, am, bm] = own[:, j * cols : (j + 1) * cols]
    for j in range(CHUNKS):
        row = []
        for k in range(1, 4):
            at = wbuf.at[j, c, am, bm]
            i = j * 3 + k - 1
            row.append(remote(at, at, gb_s.at[i], gb_r.at[i], b_peer(lax.rem(bm + k, 4))))
            row[-1].start()
        gb.append(row)
    ga = []
    for j in range(CHUNKS):
        for copy in gb[j]:
            copy.wait_recv()
        row = []
        for k in range(1, 4):
            at = wbuf.at[j, c, am]
            i = j * 3 + k - 1
            row.append(remote(at, at, ga_s.at[i], ga_r.at[i], a_peer(lax.rem(am + k, 4))))
            row[-1].start()
        ga.append(row)
    lax.fori_loop(6, blocks, turn, 0)

    gd = []

    def to_partner(j):
        for copy in ga[j]:
            copy.wait_recv()
        at = wbuf.at[j, c]
        gd.append(remote(at, at, gd_s.at[j], gd_r.at[j], partner))
        gd[-1].start()

    span = width // 16
    scale = 1.0 / rows

    def compute(j):
        for g in range(NX):
            parts = [wbuf[j, 0, g, b] for b in range(4)] + [wbuf[j, 1, b, g] for b in range(4)]
            wn[pl.ds(g * group, group)] = jnp.dot(
                perm_t[...], jnp.concatenate(parts, axis=0), preferred_element_type=F32
            ).astype(BF16)
        tile = padded // 4

        def forward(m, carry):
            at = pl.ds(pl.multiple_of(m * tile, 16), tile)
            out = jnp.dot(cbuf[at, :], wn[...], preferred_element_type=F32)
            ebuf[at, :] = (out - tbuf[j, at].astype(F32)).astype(BF16)
            return carry

        lax.fori_loop(0, 4, forward, 0)

        def backward(g, carry):
            at = pl.ds(pl.multiple_of(g * group, group), group)
            grad = jnp.dot(ct[at, :], ebuf[...], preferred_element_type=F32) * scale
            old = sbuf[j, at].astype(F32)
            chosen = []
            fresh = []
            for i in range(group // span):
                b = g * (group // span) + i
                flag = trigger[0, b].astype(F32)
                mine = grad[i * span : (i + 1) * span]
                past = old[i * span : (i + 1) * span]
                diff = mine - past
                sq = (diff * diff).reshape(span // 8, 8, cols).sum(axis=0)
                sqacc[b] = sqacc[b] + sq[:, : cols // 2] + sq[:, cols // 2 :]
                chosen.append((diff * flag).astype(BF16))
                fresh.append((flag * mine + (1.0 - flag) * past).astype(BF16))
            fbuf[j, at] = jnp.concatenate(fresh, axis=0)
            moved = jnp.dot(
                perm[...], jnp.concatenate(chosen, axis=0), preferred_element_type=F32
            ).astype(BF16)
            for b in range(4):
                half[j, 0, g, b] = moved[b * 32 : (b + 1) * 32]
                half[j, 1, b, g] = moved[128 + b * 32 : 128 + (b + 1) * 32]
            return carry

        lax.fori_loop(0, NX, backward, 0)

    rd, ra, rb, rz, fout = [], [], [], [], []

    def send_d(j):
        rd.append(remote(half.at[j, 1 - c], drecv.at[j], rd_s.at[j], rd_r.at[j], partner))
        rd[-1].start()
        fout.append(
            pltpu.make_async_copy(
                fbuf.at[j], stale_out.at[0, :, pl.ds(j * cols, cols)], fout_sem.at[j]
            )
        )
        fout[-1].start()

    def send_a(j):
        rd[j].wait_recv()
        asend[j] = (half[j, c].astype(F32) + drecv[j].astype(F32)).astype(BF16)
        row = []
        for k in range(1, 4):
            a = lax.rem(am + k, 4)
            i = j * 3 + k - 1
            row.append(
                remote(asend.at[j, a], arecv.at[j, k - 1], ra_s.at[i], ra_r.at[i], a_peer(a))
            )
            row[-1].start()
        ra.append(row)

    def send_b(j):
        for copy in ra[j]:
            copy.wait_recv()
        total = asend[j, am].astype(F32)
        for k in range(3):
            total = total + arecv[j, k].astype(F32)
        bsend[j] = total.astype(BF16)
        row = []
        for k in range(1, 4):
            b = lax.rem(bm + k, 4)
            i = j * 3 + k - 1
            row.append(
                remote(bsend.at[j, b], brecv.at[j, k - 1], rb_s.at[i], rb_r.at[i], b_peer(b))
            )
            row[-1].start()
        rb.append(row)

    def send_z(j):
        for copy in rb[j]:
            copy.wait_recv()
        total = bsend[j, bm].astype(F32)
        for k in range(3):
            total = total + brecv[j, k].astype(F32)
        for i in range(NZ):
            zsend[j, i] = total[i * PIECE : (i + 1) * PIECE]
        row = []
        for k in range(1, NZ):
            i = j * 7 + k - 1
            row.append(
                remote(
                    zsend.at[j, lax.rem(z + k, NZ)],
                    zrecv.at[j, k - 1],
                    rz_s.at[i],
                    rz_r.at[i],
                    z_peer(k),
                )
            )
            row[-1].start()
        rz.append(row)

    to_partner(0)
    for j in range(CHUNKS):
        if j + 1 < CHUNKS:
            to_partner(j + 1)
        gd[j].wait_recv()
        target_in[j].wait()
        stale_in[j].wait()
        compute(j)
        send_d(j)
        if j >= 1:
            send_a(j - 1)
        if j >= 2:
            send_b(j - 2)
        if j >= 3:
            send_z(j - 3)

    def spread(src, bufs, at, peers, first):
        out = []
        for k, to in enumerate(peers):
            out.append(remote(src, bufs.at[at], n_s.at[first + k], n_r.at[first + k], to))
            out[-1].start()
        return out

    nrm[0] = sqacc[...].sum(axis=1)
    sent = spread(nrm.at[0], nrm, 1, [partner], 0)
    last = CHUNKS - 1
    send_a(last)
    sent[0].wait_recv()
    nx_buf[x] = nrm[0] + nrm[1]
    sent_x = spread(nx_buf.at[x], nx_buf, x, [x_peer(k) for k in range(1, NX)], 1)
    send_b(last - 1)
    send_z(last - 2)
    send_b(last)
    for copy in sent_x:
        copy.wait_recv()
    ny_buf[y] = (nx_buf[0] + nx_buf[1]) + (nx_buf[2] + nx_buf[3])
    sent_y = spread(ny_buf.at[y], ny_buf, y, [y_peer(k) for k in range(1, NY)], 4)
    send_z(last - 1)
    send_z(last)
    for copy in sent_y:
        copy.wait_recv()
    nz_buf[z] = (ny_buf[0] + ny_buf[1]) + (ny_buf[2] + ny_buf[3])
    sent_z = spread(nz_buf.at[z], nz_buf, z, [z_peer(k) for k in range(1, NZ)], 7)

    for j in range(CHUNKS):
        for copy in rz[j]:
            copy.wait_recv()
        total = zsend[j, z]
        for k in range(NZ - 1):
            total = total + zrecv[j, k]
        summed_out[:, pl.ds(j * cols, cols)] = total
    for copy in sent_z:
        copy.wait_recv()
    every = nz_buf[0]
    for i in range(1, NZ):
        every = every + nz_buf[i]
    norms_out[...] = jnp.broadcast_to(jnp.sum(every, axis=1, keepdims=True), norms_out.shape)

    for copy in gz + gd + rd + sent + sent_x + sent_y + sent_z:
        copy.wait_send()
    for rows_of in (gb, ga, ra, rb, rz):
        for row in rows_of:
            for copy in row:
                copy.wait_send()
    for copy in fout:
        copy.wait()


def step(context, target, weight, stale, trigger):
    rows, width = context.shape
    cols = width // CHUNKS
    padded = -(-rows // 128) * 128
    dma = pltpu.SemaphoreType.DMA
    half = width // 2
    vmem = pl.BlockSpec(memory_space=pltpu.VMEM)
    hbm = pl.BlockSpec(memory_space=pl.ANY)
    return pl.pallas_call(
        functools.partial(step_kernel, rows, padded),
        out_shape=(
            jax.ShapeDtypeStruct((PIECE, width), F32),
            jax.ShapeDtypeStruct((1, width, width), BF16),
            jax.ShapeDtypeStruct((16, 128), F32),
        ),
        in_specs=[hbm, hbm, vmem, hbm, pl.BlockSpec(memory_space=pltpu.SMEM)],
        out_specs=(vmem, hbm, vmem),
        scratch_shapes=[
            pltpu.VMEM((padded, width), BF16),
            pltpu.VMEM((width, padded), BF16),
            pltpu.VMEM((CHUNKS, padded, cols), BF16),
            pltpu.VMEM((CHUNKS, width, cols), BF16),
            pltpu.VMEM((CHUNKS, width, cols), BF16),
            pltpu.VMEM((256, 256), BF16),
            pltpu.VMEM((256, 256), BF16),
            pltpu.VMEM((NZ, PIECE, width), F32),
            pltpu.VMEM((NZ * PIECE, width), F32),
            pltpu.VMEM((CHUNKS, 2, 4, 4, 32, cols), BF16),
            pltpu.VMEM((width, cols), BF16),
            pltpu.VMEM((padded, cols), BF16),
            pltpu.VMEM((CHUNKS, 2, 4, 4, 32, cols), BF16),
            pltpu.VMEM((CHUNKS, 4, 4, 32, cols), BF16),
            pltpu.VMEM((CHUNKS, 4, 4, 32, cols), BF16),
            pltpu.VMEM((CHUNKS, 3, 4, 32, cols), BF16),
            pltpu.VMEM((CHUNKS, 4, 32, cols), BF16),
            pltpu.VMEM((CHUNKS, 3, 32, cols), BF16),
            pltpu.VMEM((CHUNKS, NZ, PIECE, cols), F32),
            pltpu.VMEM((CHUNKS, NZ - 1, PIECE, cols), F32),
            pltpu.VMEM((16, 8, 128), F32),
            pltpu.VMEM((2, 16, 128), F32),
            pltpu.VMEM((NX, 16, 128), F32),
            pltpu.VMEM((NY, 16, 128), F32),
            pltpu.VMEM((NZ, 16, 128), F32),
            dma,
            dma((CHUNKS,)),
            dma((CHUNKS,)),
            dma((CHUNKS,)),
            dma((NZ - 1,)),
            dma((NZ - 1,)),
            dma((CHUNKS * 3,)),
            dma((CHUNKS * 3,)),
            dma((CHUNKS * 3,)),
            dma((CHUNKS * 3,)),
            dma((CHUNKS,)),
            dma((CHUNKS,)),
            dma((CHUNKS,)),
            dma((CHUNKS,)),
            dma((CHUNKS * 3,)),
            dma((CHUNKS * 3,)),
            dma((CHUNKS * 3,)),
            dma((CHUNKS * 3,)),
            dma((CHUNKS * 7,)),
            dma((CHUNKS * 7,)),
            dma((14,)),
            dma((14,)),
        ],
        compiler_params=pltpu.CompilerParams(
            collective_id=0, has_side_effects=True, vmem_limit_bytes=60 * 1024 * 1024
        ),
        name="step",
    )(context, target, weight, stale, trigger)


def body(context, target, weight, stale, trigger, aggregate, moment, second):
    summed, stale_new, norms = step(context, target, weight, stale, trigger)
    aggregate_new = aggregate + summed
    moment_new = 0.9 * moment + 0.1 * aggregate_new
    second_new = 0.999 * second + 0.001 * aggregate_new * aggregate_new
    weight_new = weight - 0.001 * (moment_new / (jnp.sqrt(second_new) + 1e-08) + 0.05 * weight)
    return (aggregate_new, weight_new, moment_new, second_new, stale_new, norms[:, 0])


def solution(mesh):
    split = P(("dp", "sub"), None)
    return jax.shard_map(
        body,
        mesh=mesh,
        in_specs=(split, split, split, P(("dp", "sub"), None, None), split, split, split, split),
        out_specs=(split, split, split, split, P(("dp", "sub"), None, None), P()),
        check_vma=False,
    )
```

```python
import functools

import jax
import jax.numpy as jnp
from jax import lax
from jax.experimental import pallas as pl
from jax.experimental.pallas import tpu as pltpu
from jax.sharding import PartitionSpec as P

MESH = pl.DeviceIdType.MESH
F32 = jnp.float32
BF16 = jnp.bfloat16
CHUNKS = 4
NX = 4
NY = 4
NZ = 8
PIECE = 4


def step_kernel(
    rows,
    padded,
    context,
    target,
    weight,
    stale,
    trigger,
    summed_out,
    stale_out,
    norms_out,
    cbuf,
    ct,
    tbuf,
    sbuf,
    fbuf,
    perm,
    perm_t,
    wz,
    wz32,
    wbuf,
    own_low,
    ebuf,
    half,
    drecv,
    asend,
    arecv,
    bsend,
    brecv,
    zsend,
    zrecv,
    sqacc,
    flags,
    nrm,
    nx_buf,
    ny_buf,
    nz_buf,
    cin_sem,
    tin_sem,
    sin_sem,
    gz_s,
    gz_r,
    gb_s,
    gb_r,
    ga_s,
    ga_r,
    gd_s,
    gd_r,
    rd_s,
    rd_r,
    ra_s,
    ra_r,
    rb_s,
    rb_r,
    rz_s,
    rz_r,
    n_s,
    n_r,
):
    width = context.shape[1]
    cols = width // CHUNKS
    dp = lax.axis_index("dp")
    sub = lax.axis_index("sub")
    c = lax.rem(dp, 2)
    x = lax.div(dp, 8)
    zlo = lax.rem(lax.div(dp, 2), 4)
    zhi = lax.div(sub, NY)
    y = lax.rem(sub, NY)
    z = zhi * 4 + zlo
    am = x * (1 - c) + y * c
    bm = y * (1 - c) + x * c

    def device(px, py, pz, pc):
        return ((px * 4 + lax.rem(pz, 4)) * 2 + pc, lax.div(pz, 4) * NY + py)

    def a_peer(a):
        return device(a * (1 - c) + x * c, y * (1 - c) + a * c, z, c)

    def b_peer(b):
        return device(x * (1 - c) + b * c, b * (1 - c) + y * c, z, c)

    def x_peer(k):
        return device(lax.rem(x + k, NX), y, z, c)

    def y_peer(k):
        return device(x, lax.rem(y + k, NY), z, c)

    def z_peer(k):
        return device(x, y, lax.rem(z + k, NZ), c)

    partner = device(x, y, z, 1 - c)

    def remote(src, dst, s, r, to):
        return pltpu.make_async_remote_copy(
            src_ref=src, dst_ref=dst, send_sem=s, recv_sem=r, device_id=to, device_id_type=MESH
        )

    context_in = pltpu.make_async_copy(context, cbuf.at[pl.ds(0, rows)], cin_sem)
    context_in.start()
    target_in = []
    stale_in = []
    for j in range(CHUNKS):
        part = pl.ds(j * cols, cols)
        target_in.append(
            pltpu.make_async_copy(target.at[:, part], tbuf.at[j, pl.ds(0, rows)], tin_sem.at[j])
        )
        stale_in.append(pltpu.make_async_copy(stale.at[0, :, part], sbuf.at[j], sin_sem.at[j]))
        target_in[j].start()
        stale_in[j].start()

    barrier = pltpu.get_barrier_semaphore()
    greeted = [partner]
    greeted += [x_peer(k) for k in range(1, NX)]
    greeted += [y_peer(k) for k in range(1, NY)]
    greeted += [z_peer(k) for k in range(1, NZ)]
    for to in greeted:
        pl.semaphore_signal(barrier, inc=1, device_id=to, device_id_type=MESH)

    group = 2 * NY * NZ * PIECE
    place = lax.broadcasted_iota(jnp.int32, (group, group), 0)
    natural = lax.broadcasted_iota(jnp.int32, (group, group), 1)

    def natural_of(i):
        ic, iy, iz, ir = i // 128, (i // 32) % 4, (i // 4) % 8, i % 4
        return (iz % 4) * 64 + ic * 32 + (iz // 4) * 16 + iy * 4 + ir

    perm[...] = jnp.where(natural == natural_of(place), 1.0, 0.0).astype(BF16)
    perm_t[...] = jnp.where(place == natural_of(natural), 1.0, 0.0).astype(BF16)
    own_low[...] = weight[...].astype(BF16)
    tail = padded - rows
    cbuf[pl.ds(rows, tail)] = jnp.zeros((tail, width), BF16)
    ebuf[...] = jnp.zeros((padded, cols), BF16)
    for j in range(CHUNKS):
        tbuf[j, pl.ds(rows, tail)] = jnp.zeros((tail, cols), BF16)
    sqacc[...] = jnp.zeros(sqacc.shape, F32)

    pl.semaphore_wait(barrier, len(greeted))

    gz = []
    for k in range(1, NZ):
        gz.append(remote(own_low, wz.at[z], gz_s.at[k - 1], gz_r.at[k - 1], z_peer(k)))
        gz[-1].start()
    wz[z] = own_low[...]
    context_in.wait()

    def turn(m, carry):
        span = pl.ds(pl.multiple_of(m * 128, 128), 128)
        for g in range(NX):
            at = pl.ds(g * group, group)
            moved = jnp.dot(cbuf[span, at], perm_t[...], preferred_element_type=F32).astype(BF16)
            cbuf[span, at] = moved
            ct[at, span] = moved.T
        return carry

    lax.fori_loop(0, padded // 128, turn, 0)
    for copy in gz:
        copy.wait_recv()
    for i in range(NZ):
        wz32[pl.ds(i * PIECE, PIECE), :] = wz[i].astype(F32)
    own = wz32[...].astype(BF16)
    gb = []
    for j in range(CHUNKS):
        wbuf[j, c, am, bm] = own[:, j * cols : (j + 1) * cols]
    for j in range(CHUNKS):
        row = []
        for k in range(1, 4):
            at = wbuf.at[j, c, am, bm]
            i = j * 3 + k - 1
            row.append(remote(at, at, gb_s.at[i], gb_r.at[i], b_peer(lax.rem(bm + k, 4))))
            row[-1].start()
        gb.append(row)
    ga = []
    for j in range(CHUNKS):
        for copy in gb[j]:
            copy.wait_recv()
        row = []
        for k in range(1, 4):
            at = wbuf.at[j, c, am]
            i = j * 3 + k - 1
            row.append(remote(at, at, ga_s.at[i], ga_r.at[i], a_peer(lax.rem(am + k, 4))))
            row[-1].start()
        ga.append(row)
    for j in range(CHUNKS):
        stale_in[j].wait()
        for g in range(NX):
            at = pl.ds(g * group, group)
            sbuf[j, at] = jnp.dot(perm[...], sbuf[j, at], preferred_element_type=F32).astype(BF16)
    low = lax.broadcasted_iota(jnp.int32, (16, cols), 0) // PIECE
    for g in range(NX):
        flag = jnp.zeros((16, cols), F32)
        for i in range(4):
            flag = jnp.where(low == i, trigger[0, g * 4 + i].astype(F32), flag)
        flags[g] = flag

    gd = []

    def to_partner(j):
        for copy in ga[j]:
            copy.wait_recv()
        at = wbuf.at[j, c]
        gd.append(remote(at, at, gd_s.at[j], gd_r.at[j], partner))
        gd[-1].start()

    scale = 1.0 / rows
    tile = padded // 4

    def forward(j):
        parts = []
        for g in range(NX):
            parts += [wbuf[j, 0, g, b] for b in range(4)] + [wbuf[j, 1, b, g] for b in range(4)]
        low_part = jnp.concatenate(parts, axis=0)
        for m in range(4):
            at = pl.ds(m * tile, tile)
            out = jnp.dot(cbuf[at, :], low_part, preferred_element_type=F32)
            ebuf[at, :] = (out - tbuf[j, at].astype(F32)).astype(BF16)

    def backward(j):
        for g in range(NX):
            at = pl.ds(g * group, group)
            grad = jnp.dot(ct[at, :], ebuf[...], preferred_element_type=F32) * scale
            mine = grad.reshape(16, 16, cols)
            past = sbuf[j, at].astype(F32).reshape(16, 16, cols)
            flag = flags[g][None]
            diff = mine - past
            sq = (diff * diff).sum(axis=0)
            sqacc[g] = sqacc[g] + sq[:, : cols // 2] + sq[:, cols // 2 :]
            chosen = (diff * flag).reshape(group, cols).astype(BF16)
            fresh = flag * mine + (1.0 - flag) * past
            fbuf[j, at] = fresh.reshape(group, cols).astype(BF16)
            for b in range(4):
                half[j, 0, g, b] = chosen[b * 32 : (b + 1) * 32]
                half[j, 1, b, g] = chosen[128 + b * 32 : 128 + (b + 1) * 32]

    def finish(j):
        for g in range(NX):
            at = pl.ds(g * group, group)
            stale_out[0, at, pl.ds(j * cols, cols)] = jnp.dot(
                perm_t[...], fbuf[j, at], preferred_element_type=F32
            ).astype(BF16)

    rd, ra, rb, rz = [], [], [], []

    def send_d(j):
        rd.append(remote(half.at[j, 1 - c], drecv.at[j], rd_s.at[j], rd_r.at[j], partner))
        rd[-1].start()

    def send_a(j):
        rd[j].wait_recv()
        asend[j] = (half[j, c].astype(F32) + drecv[j].astype(F32)).astype(BF16)
        row = []
        for k in range(1, 4):
            a = lax.rem(am + k, 4)
            i = j * 3 + k - 1
            row.append(
                remote(asend.at[j, a], arecv.at[j, k - 1], ra_s.at[i], ra_r.at[i], a_peer(a))
            )
            row[-1].start()
        ra.append(row)

    def send_b(j):
        for copy in ra[j]:
            copy.wait_recv()
        total = asend[j, am].astype(F32)
        for k in range(3):
            total = total + arecv[j, k].astype(F32)
        bsend[j] = total.astype(BF16)
        row = []
        for k in range(1, 4):
            b = lax.rem(bm + k, 4)
            i = j * 3 + k - 1
            row.append(
                remote(bsend.at[j, b], brecv.at[j, k - 1], rb_s.at[i], rb_r.at[i], b_peer(b))
            )
            row[-1].start()
        rb.append(row)

    def send_z(j):
        for copy in rb[j]:
            copy.wait_recv()
        total = bsend[j, bm].astype(F32)
        for k in range(3):
            total = total + brecv[j, k].astype(F32)
        for i in range(NZ):
            zsend[j, i] = total[i * PIECE : (i + 1) * PIECE].astype(BF16)
        row = []
        for k in range(1, NZ):
            i = j * 7 + k - 1
            row.append(
                remote(
                    zsend.at[j, lax.rem(z + k, NZ)],
                    zrecv.at[j, k - 1],
                    rz_s.at[i],
                    rz_r.at[i],
                    z_peer(k),
                )
            )
            row[-1].start()
        rz.append(row)

    to_partner(0)
    for j in range(CHUNKS):
        gd[j].wait_recv()
        target_in[j].wait()
        forward(j)
        if j + 1 < CHUNKS:
            to_partner(j + 1)
        if j >= 1:
            send_a(j - 1)
        if j >= 3:
            send_b(j - 3)
        backward(j)
        send_d(j)

    def spread(src, bufs, at, peers, first):
        out = []
        for k, to in enumerate(peers):
            out.append(remote(src, bufs.at[at], n_s.at[first + k], n_r.at[first + k], to))
            out[-1].start()
        return out

    pick = lax.broadcasted_iota(jnp.int32, (16, 64), 1) // PIECE
    pick = jnp.where(pick == lax.broadcasted_iota(jnp.int32, (16, 64), 0), 1.0, 0.0)
    nrm[0] = jnp.dot(
        pick.astype(F32),
        sqacc[...].reshape(64, 128),
        precision=lax.Precision.HIGHEST,
        preferred_element_type=F32,
    )
    sent = spread(nrm.at[0], nrm, 1, [partner], 0)
    send_b(1)
    send_z(0)
    send_a(3)
    sent[0].wait_recv()
    nx_buf[x] = nrm[0] + nrm[1]
    sent_x = spread(nx_buf.at[x], nx_buf, x, [x_peer(k) for k in range(1, NX)], 1)
    send_z(1)
    finish(0)
    finish(1)
    send_b(2)
    finish(2)
    finish(3)
    send_b(3)
    for copy in sent_x:
        copy.wait_recv()
    ny_buf[y] = (nx_buf[0] + nx_buf[1]) + (nx_buf[2] + nx_buf[3])
    sent_y = spread(ny_buf.at[y], ny_buf, y, [y_peer(k) for k in range(1, NY)], 4)
    send_z(2)
    send_z(3)
    for copy in sent_y:
        copy.wait_recv()
    nz_buf[z] = (ny_buf[0] + ny_buf[1]) + (ny_buf[2] + ny_buf[3])
    sent_z = spread(nz_buf.at[z], nz_buf, z, [z_peer(k) for k in range(1, NZ)], 7)

    for j in range(CHUNKS):
        for copy in rz[j]:
            copy.wait_recv()
        total = zsend[j, z].astype(F32)
        for k in range(NZ - 1):
            total = total + zrecv[j, k].astype(F32)
        summed_out[:, pl.ds(j * cols, cols)] = total
    for copy in sent_z:
        copy.wait_recv()
    every = nz_buf[0]
    for i in range(1, NZ):
        every = every + nz_buf[i]
    sums = jnp.broadcast_to(jnp.sum(every, axis=1, keepdims=True), (16, 128))
    row = lax.broadcasted_iota(jnp.int32, (16, 128), 0)
    lane = lax.broadcasted_iota(jnp.int32, (16, 128), 1)
    norms_out[...] = jnp.sum(jnp.where(row == lane, sums, 0.0), axis=0, keepdims=True)

    for copy in gz + gd + rd + sent + sent_x + sent_y + sent_z:
        copy.wait_send()
    for rows_of in (gb, ga, ra, rb, rz):
        for row in rows_of:
            for copy in row:
                copy.wait_send()


def step(context, target, weight, stale, trigger):
    rows, width = context.shape
    cols = width // CHUNKS
    padded = -(-rows // 128) * 128
    dma = pltpu.SemaphoreType.DMA
    vmem = pl.BlockSpec(memory_space=pltpu.VMEM)
    hbm = pl.BlockSpec(memory_space=pltpu.HBM)
    return pl.pallas_call(
        functools.partial(step_kernel, rows, padded),
        out_shape=(
            jax.ShapeDtypeStruct((PIECE, width), F32),
            jax.ShapeDtypeStruct((1, width, width), BF16),
            jax.ShapeDtypeStruct((1, 128), F32),
        ),
        in_specs=[hbm, hbm, vmem, hbm, pl.BlockSpec(memory_space=pltpu.SMEM)],
        out_specs=(vmem, vmem, vmem),
        scratch_shapes=[
            pltpu.VMEM((padded, width), BF16),
            pltpu.VMEM((width, padded), BF16),
            pltpu.VMEM((CHUNKS, padded, cols), BF16),
            pltpu.VMEM((CHUNKS, width, cols), BF16),
            pltpu.VMEM((CHUNKS, width, cols), BF16),
            pltpu.VMEM((256, 256), BF16),
            pltpu.VMEM((256, 256), BF16),
            pltpu.VMEM((NZ, PIECE, width), BF16),
            pltpu.VMEM((NZ * PIECE, width), F32),
            pltpu.VMEM((CHUNKS, 2, 4, 4, 32, cols), BF16),
            pltpu.VMEM((PIECE, width), BF16),
            pltpu.VMEM((padded, cols), BF16),
            pltpu.VMEM((CHUNKS, 2, 4, 4, 32, cols), BF16),
            pltpu.VMEM((CHUNKS, 4, 4, 32, cols), BF16),
            pltpu.VMEM((CHUNKS, 4, 4, 32, cols), BF16),
            pltpu.VMEM((CHUNKS, 3, 4, 32, cols), BF16),
            pltpu.VMEM((CHUNKS, 4, 32, cols), BF16),
            pltpu.VMEM((CHUNKS, 3, 32, cols), BF16),
            pltpu.VMEM((CHUNKS, NZ, PIECE, cols), BF16),
            pltpu.VMEM((CHUNKS, NZ - 1, PIECE, cols), BF16),
            pltpu.VMEM((4, 16, 128), F32),
            pltpu.VMEM((4, 16, cols), F32),
            pltpu.VMEM((2, 16, 128), F32),
            pltpu.VMEM((NX, 16, 128), F32),
            pltpu.VMEM((NY, 16, 128), F32),
            pltpu.VMEM((NZ, 16, 128), F32),
            dma,
            dma((CHUNKS,)),
            dma((CHUNKS,)),
            dma((NZ - 1,)),
            dma((NZ - 1,)),
            dma((CHUNKS * 3,)),
            dma((CHUNKS * 3,)),
            dma((CHUNKS * 3,)),
            dma((CHUNKS * 3,)),
            dma((CHUNKS,)),
            dma((CHUNKS,)),
            dma((CHUNKS,)),
            dma((CHUNKS,)),
            dma((CHUNKS * 3,)),
            dma((CHUNKS * 3,)),
            dma((CHUNKS * 3,)),
            dma((CHUNKS * 3,)),
            dma((CHUNKS * 7,)),
            dma((CHUNKS * 7,)),
            dma((14,)),
            dma((14,)),
        ],
        compiler_params=pltpu.CompilerParams(
            collective_id=0, has_side_effects=True, vmem_limit_bytes=50 * 1024 * 1024
        ),
        name="step",
    )(context, target, weight, stale, trigger)


def body(context, target, weight, stale, trigger, aggregate, moment, second):
    summed, stale_new, norms = step(context, target, weight, stale, trigger)
    aggregate_new = aggregate + summed
    moment_new = 0.9 * moment + 0.1 * aggregate_new
    second_new = 0.999 * second + 0.001 * aggregate_new * aggregate_new
    weight_new = weight - 0.001 * (moment_new / (jnp.sqrt(second_new) + 1e-08) + 0.05 * weight)
    return (aggregate_new, weight_new, moment_new, second_new, stale_new, norms[0, :16])


def solution(mesh):
    split = P(("dp", "sub"), None)
    return jax.shard_map(
        body,
        mesh=mesh,
        in_specs=(split, split, split, P(("dp", "sub"), None, None), split, split, split, split),
        out_specs=(split, split, split, split, P(("dp", "sub"), None, None), P()),
        check_vma=False,
    )
```

```python
import functools

import jax
import jax.numpy as jnp
from jax import lax
from jax.experimental import pallas as pl
from jax.experimental.pallas import tpu as pltpu
from jax.sharding import PartitionSpec as P

MESH = pl.DeviceIdType.MESH
F32 = jnp.float32
BF16 = jnp.bfloat16
CHUNKS = 4
NX = 4
NY = 4
NZ = 8
PIECE = 4


def step_kernel(
    rows,
    padded,
    context,
    target,
    small,
    stale,
    summed_out,
    stale_out,
    norms_out,
    cbuf,
    ct,
    tbuf,
    sbuf,
    fbuf,
    perm,
    perm_t,
    wz,
    wz32,
    wbuf,
    own_low,
    ebuf,
    half,
    drecv,
    asend,
    arecv,
    bsend,
    brecv,
    zsend,
    zrecv,
    sqacc,
    flags,
    nrm,
    nx_buf,
    ny_buf,
    nz_buf,
    cin_sem,
    tin_sem,
    sin_sem,
    gz_s,
    gz_r,
    gb_s,
    gb_r,
    ge_s,
    ge_r,
    ga_s,
    ga_r,
    gd_s,
    gd_r,
    rd_s,
    rd_r,
    ra_s,
    ra_r,
    rb_s,
    rb_r,
    rz_s,
    rz_r,
    n_s,
    n_r,
):
    width = context.shape[1]
    cols = width // CHUNKS
    dp = lax.axis_index("dp")
    sub = lax.axis_index("sub")
    c = lax.rem(dp, 2)
    x = lax.div(dp, 8)
    zlo = lax.rem(lax.div(dp, 2), 4)
    zhi = lax.div(sub, NY)
    y = lax.rem(sub, NY)
    z = zhi * 4 + zlo
    am = x * (1 - c) + y * c
    bm = y * (1 - c) + x * c

    def device(px, py, pz, pc):
        return ((px * 4 + lax.rem(pz, 4)) * 2 + pc, lax.div(pz, 4) * NY + py)

    def a_peer(a):
        return device(a * (1 - c) + x * c, y * (1 - c) + a * c, z, c)

    def b_peer(b):
        return device(x * (1 - c) + b * c, b * (1 - c) + y * c, z, c)

    def x_peer(k):
        return device(lax.rem(x + k, NX), y, z, c)

    def y_peer(k):
        return device(x, lax.rem(y + k, NY), z, c)

    def z_peer(k):
        return device(x, y, lax.rem(z + k, NZ), c)

    partner = device(x, y, z, 1 - c)

    def remote(src, dst, s, r, to):
        return pltpu.make_async_remote_copy(
            src_ref=src, dst_ref=dst, send_sem=s, recv_sem=r, device_id=to, device_id_type=MESH
        )

    barrier = pltpu.get_barrier_semaphore()
    greeted = [partner]
    greeted += [x_peer(k) for k in range(1, NX)]
    greeted += [y_peer(k) for k in range(1, NY)]
    greeted += [z_peer(k) for k in range(1, NZ)]
    for to in greeted:
        pl.semaphore_signal(barrier, inc=1, device_id=to, device_id_type=MESH)

    context_in = pltpu.make_async_copy(context, cbuf.at[pl.ds(0, rows)], cin_sem)
    context_in.start()
    target_in = []
    stale_in = []
    for j in range(CHUNKS):
        part = pl.ds(j * cols, cols)
        target_in.append(
            pltpu.make_async_copy(target.at[:, part], tbuf.at[j, pl.ds(0, rows)], tin_sem.at[j])
        )
        stale_in.append(pltpu.make_async_copy(stale.at[0, :, part], sbuf.at[j], sin_sem.at[j]))
        target_in[j].start()
        stale_in[j].start()

    own_low[...] = small[:PIECE].astype(BF16)
    pl.semaphore_wait(barrier, len(greeted))

    gz = []
    for k in range(1, NZ):
        gz.append(remote(own_low, wz.at[z], gz_s.at[k - 1], gz_r.at[k - 1], z_peer(k)))
        gz[-1].start()
    wz[z] = own_low[...]

    group = 2 * NY * NZ * PIECE
    place = lax.broadcasted_iota(jnp.int32, (group, group), 0)
    natural = lax.broadcasted_iota(jnp.int32, (group, group), 1)

    def natural_of(i):
        ic, iy, iz, ir = i // 128, (i // 32) % 4, (i // 4) % 8, i % 4
        return (iz % 4) * 64 + ic * 32 + (iz // 4) * 16 + iy * 4 + ir

    perm[...] = jnp.where(natural == natural_of(place), 1.0, 0.0).astype(BF16)
    perm_t[...] = jnp.where(place == natural_of(natural), 1.0, 0.0).astype(BF16)
    tail = padded - rows
    cbuf[pl.ds(rows, tail)] = jnp.zeros((tail, width), BF16)
    ebuf[...] = jnp.zeros((padded, cols), BF16)
    for j in range(CHUNKS):
        tbuf[j, pl.ds(rows, tail)] = jnp.zeros((tail, cols), BF16)
    sqacc[...] = jnp.zeros(sqacc.shape, F32)

    context_in.wait()

    def turn(m, carry):
        span = pl.ds(pl.multiple_of(m * 128, 128), 128)
        for g in range(NX):
            at = pl.ds(g * group, group)
            moved = jnp.dot(cbuf[span, at], perm_t[...], preferred_element_type=F32).astype(BF16)
            cbuf[span, at] = moved
            ct[at, span] = moved.T
        return carry

    lax.fori_loop(0, padded // 128, turn, 0)
    for copy in gz:
        copy.wait_recv()
    for i in range(NZ):
        wz32[pl.ds(i * PIECE, PIECE), :] = wz[i].astype(F32)
    own = wz32[...].astype(BF16)
    gb = []
    for j in range(CHUNKS):
        wbuf[j, c, am, 0] = own[:, j * cols : (j + 1) * cols]
    for j in range(CHUNKS):
        row = []
        for k in range(1, 4):
            i = j * 3 + k - 1
            row.append(
                remote(
                    wbuf.at[j, c, am, 0],
                    wbuf.at[j, c, am, 4 - k],
                    gb_s.at[i],
                    gb_r.at[i],
                    b_peer(lax.rem(bm + k, 4)),
                )
            )
            row[-1].start()
        gb.append(row)
    ge = []
    for k in range(1, 4):
        at = wbuf.at[:, c, am, 0]
        ge.append(remote(at, at, ge_s.at[k - 1], ge_r.at[k - 1], a_peer(lax.rem(am + k, 4))))
        ge[-1].start()
    ga = []
    for j in range(CHUNKS):
        for copy in gb[j]:
            copy.wait_recv()
        row = []
        for k in range(1, 4):
            at = wbuf.at[j, c, am, pl.ds(1, 3)]
            i = j * 3 + k - 1
            row.append(remote(at, at, ga_s.at[i], ga_r.at[i], a_peer(lax.rem(am + k, 4))))
            row[-1].start()
        ga.append(row)
    for j in range(CHUNKS):
        stale_in[j].wait()
        for g in range(NX):
            at = pl.ds(g * group, group)
            sbuf[j, at] = jnp.dot(perm[...], sbuf[j, at], preferred_element_type=F32).astype(BF16)
    low = lax.broadcasted_iota(jnp.int32, (16, cols), 0) // PIECE
    marks = small[PIECE : PIECE + 1, :128]
    mark_at = lax.broadcasted_iota(jnp.int32, (1, 128), 1)
    for g in range(NX):
        flag = jnp.zeros((16, cols), F32)
        for i in range(4):
            one = jnp.sum(
                jnp.where(mark_at == g * 4 + i, marks, 0.0), axis=1, keepdims=True
            )
            flag = jnp.where(low == i, one, flag)
        flags[g] = flag

    gd = []

    def to_partner(j):
        for copy in ga[j]:
            copy.wait_recv()
        at = wbuf.at[j, c]
        gd.append(remote(at, at, gd_s.at[j], gd_r.at[j], partner))
        gd[-1].start()

    scale = 1.0 / rows
    tile = padded // 4

    def forward(j):
        parts = []
        for g in range(NX):
            parts += [wbuf[j, 0, g, lax.rem(b - y + 4, 4)] for b in range(4)]
            parts += [wbuf[j, 1, b, lax.rem(g - x + 4, 4)] for b in range(4)]
        low_part = jnp.concatenate(parts, axis=0)
        for m in range(4):
            at = pl.ds(m * tile, tile)
            out = jnp.dot(cbuf[at, :], low_part, preferred_element_type=F32)
            ebuf[at, :] = (out - tbuf[j, at].astype(F32)).astype(BF16)

    def backward(j, first, last):
        for g in range(first, last):
            at = pl.ds(g * group, group)
            grad = jnp.dot(ct[at, :], ebuf[...], preferred_element_type=F32) * scale
            mine = grad.reshape(16, 16, cols)
            past = sbuf[j, at].astype(F32).reshape(16, 16, cols)
            flag = flags[g][None]
            diff = mine - past
            sq = (diff * diff).sum(axis=0)
            sqacc[g] = sqacc[g] + sq[:, : cols // 2] + sq[:, cols // 2 :]
            chosen = (diff * flag).reshape(group, cols).astype(BF16)
            fresh = flag * mine + (1.0 - flag) * past
            fbuf[j, at] = fresh.reshape(group, cols).astype(BF16)
            for b in range(4):
                half[j, 0, g, b] = chosen[b * 32 : (b + 1) * 32]
                half[j, 1, g, b] = chosen[128 + b * 32 : 128 + (b + 1) * 32]

    def finish(j):
        for g in range(NX):
            at = pl.ds(g * group, group)
            stale_out[0, at, pl.ds(j * cols, cols)] = jnp.dot(
                perm_t[...], fbuf[j, at], preferred_element_type=F32
            ).astype(BF16)

    rd, ra, rb, rz = [], [], [], []

    def send_d(j, first, last):
        for g in range(first, last):
            rd.append(
                remote(
                    half.at[j, 1 - c, g],
                    drecv.at[j, g],
                    rd_s.at[j * NX + g],
                    rd_r.at[j * NX + g],
                    partner,
                )
            )
            rd[-1].start()

    def send_a(j):
        for g in range(NX):
            rd[j * NX + g].wait_recv()
            for b in range(4):
                both = half[j, c, g, b].astype(F32) + drecv[j, g, b].astype(F32)
                asend[j, g * (1 - c) + b * c, b * (1 - c) + g * c] = both.astype(BF16)
        row = []
        for k in range(1, 4):
            a = lax.rem(am + k, 4)
            i = j * 3 + k - 1
            row.append(
                remote(asend.at[j, a], arecv.at[j, k - 1], ra_s.at[i], ra_r.at[i], a_peer(a))
            )
            row[-1].start()
        ra.append(row)

    def send_b(j):
        for copy in ra[j]:
            copy.wait_recv()
        total = asend[j, am].astype(F32)
        for k in range(3):
            total = total + arecv[j, k].astype(F32)
        bsend[j] = total.astype(BF16)
        row = []
        for k in range(1, 4):
            b = lax.rem(bm + k, 4)
            i = j * 3 + k - 1
            row.append(
                remote(bsend.at[j, b], brecv.at[j, k - 1], rb_s.at[i], rb_r.at[i], b_peer(b))
            )
            row[-1].start()
        rb.append(row)

    def send_z(j):
        for copy in rb[j]:
            copy.wait_recv()
        total = bsend[j, bm].astype(F32)
        for k in range(3):
            total = total + brecv[j, k].astype(F32)
        for i in range(NZ):
            zsend[j, i] = total[i * PIECE : (i + 1) * PIECE].astype(BF16)
        row = []
        for k in range(1, NZ):
            i = j * 7 + k - 1
            row.append(
                remote(
                    zsend.at[j, lax.rem(z + k, NZ)],
                    zrecv.at[j, k - 1],
                    rz_s.at[i],
                    rz_r.at[i],
                    z_peer(k),
                )
            )
            row[-1].start()
        rz.append(row)

    for copy in ge:
        copy.wait_recv()
    to_partner(0)
    for j in range(CHUNKS):
        gd[j].wait_recv()
        target_in[j].wait()
        forward(j)
        if j + 1 < CHUNKS:
            to_partner(j + 1)
        if j >= 1:
            send_a(j - 1)
        if j >= 3:
            send_b(j - 3)
        if j < CHUNKS - 1:
            backward(j, 0, NX)
            send_d(j, 0, NX)
        else:
            backward(j, 0, 2)
            send_d(j, 0, 2)
            backward(j, 2, NX)
            send_d(j, 2, NX)

    def spread(src, bufs, at, peers, first):
        out = []
        for k, to in enumerate(peers):
            out.append(remote(src, bufs.at[at], n_s.at[first + k], n_r.at[first + k], to))
            out[-1].start()
        return out

    pick = lax.broadcasted_iota(jnp.int32, (16, 64), 1) // PIECE
    pick = jnp.where(pick == lax.broadcasted_iota(jnp.int32, (16, 64), 0), 1.0, 0.0)
    nrm[0] = jnp.dot(
        pick.astype(F32),
        sqacc[...].reshape(64, 128),
        precision=lax.Precision.HIGHEST,
        preferred_element_type=F32,
    )
    sent = spread(nrm.at[0], nrm, 1, [partner], 0)
    send_a(3)
    sent[0].wait_recv()
    nx_buf[x] = nrm[0] + nrm[1]
    sent_x = spread(nx_buf.at[x], nx_buf, x, [x_peer(k) for k in range(1, NX)], 1)
    send_b(1)
    send_z(0)
    finish(0)
    finish(1)
    send_b(2)
    finish(2)
    send_z(1)
    finish(3)
    send_b(3)
    for copy in sent_x:
        copy.wait_recv()
    ny_buf[y] = (nx_buf[0] + nx_buf[1]) + (nx_buf[2] + nx_buf[3])
    sent_y = spread(ny_buf.at[y], ny_buf, y, [y_peer(k) for k in range(1, NY)], 4)
    send_z(2)
    send_z(3)
    for copy in sent_y:
        copy.wait_recv()
    nz_buf[z] = (ny_buf[0] + ny_buf[1]) + (ny_buf[2] + ny_buf[3])
    sent_z = spread(nz_buf.at[z], nz_buf, z, [z_peer(k) for k in range(1, NZ)], 7)

    for j in range(CHUNKS):
        for copy in rz[j]:
            copy.wait_recv()
        total = zsend[j, z].astype(F32)
        for k in range(NZ - 1):
            total = total + zrecv[j, k].astype(F32)
        summed_out[:, pl.ds(j * cols, cols)] = total
    for copy in sent_z:
        copy.wait_recv()
    every = nz_buf[0]
    for i in range(1, NZ):
        every = every + nz_buf[i]
    sums = jnp.broadcast_to(jnp.sum(every, axis=1, keepdims=True), (16, 128))
    row = lax.broadcasted_iota(jnp.int32, (16, 128), 0)
    lane = lax.broadcasted_iota(jnp.int32, (16, 128), 1)
    norms_out[...] = jnp.sum(jnp.where(row == lane, sums, 0.0), axis=0, keepdims=True)

    for copy in gz + ge + gd + rd + sent + sent_x + sent_y + sent_z:
        copy.wait_send()
    for rows_of in (gb, ga, ra, rb, rz):
        for row in rows_of:
            for copy in row:
                copy.wait_send()


def step(context, target, small, stale):
    rows, width = context.shape
    cols = width // CHUNKS
    padded = -(-rows // 128) * 128
    dma = pltpu.SemaphoreType.DMA
    vmem = pl.BlockSpec(memory_space=pltpu.VMEM)
    hbm = pl.BlockSpec(memory_space=pltpu.HBM)
    return pl.pallas_call(
        functools.partial(step_kernel, rows, padded),
        out_shape=(
            jax.ShapeDtypeStruct((PIECE, width), F32),
            jax.ShapeDtypeStruct((1, width, width), BF16),
            jax.ShapeDtypeStruct((1, 128), F32),
        ),
        in_specs=[hbm, hbm, vmem, hbm],
        out_specs=(vmem, vmem, vmem),
        scratch_shapes=[
            pltpu.VMEM((padded, width), BF16),
            pltpu.VMEM((width, padded), BF16),
            pltpu.VMEM((CHUNKS, padded, cols), BF16),
            pltpu.VMEM((CHUNKS, width, cols), BF16),
            pltpu.VMEM((CHUNKS, width, cols), BF16),
            pltpu.VMEM((256, 256), BF16),
            pltpu.VMEM((256, 256), BF16),
            pltpu.VMEM((NZ, PIECE, width), BF16),
            pltpu.VMEM((NZ * PIECE, width), F32),
            pltpu.VMEM((CHUNKS, 2, 4, 4, 32, cols), BF16),
            pltpu.VMEM((PIECE, width), BF16),
            pltpu.VMEM((padded, cols), BF16),
            pltpu.VMEM((CHUNKS, 2, 4, 4, 32, cols), BF16),
            pltpu.VMEM((CHUNKS, 4, 4, 32, cols), BF16),
            pltpu.VMEM((CHUNKS, 4, 4, 32, cols), BF16),
            pltpu.VMEM((CHUNKS, 3, 4, 32, cols), BF16),
            pltpu.VMEM((CHUNKS, 4, 32, cols), BF16),
            pltpu.VMEM((CHUNKS, 3, 32, cols), BF16),
            pltpu.VMEM((CHUNKS, NZ, PIECE, cols), BF16),
            pltpu.VMEM((CHUNKS, NZ - 1, PIECE, cols), BF16),
            pltpu.VMEM((4, 16, 128), F32),
            pltpu.VMEM((4, 16, cols), F32),
            pltpu.VMEM((2, 16, 128), F32),
            pltpu.VMEM((NX, 16, 128), F32),
            pltpu.VMEM((NY, 16, 128), F32),
            pltpu.VMEM((NZ, 16, 128), F32),
            dma,
            dma((CHUNKS,)),
            dma((CHUNKS,)),
            dma((NZ - 1,)),
            dma((NZ - 1,)),
            dma((CHUNKS * 3,)),
            dma((CHUNKS * 3,)),
            dma((3,)),
            dma((3,)),
            dma((CHUNKS * 3,)),
            dma((CHUNKS * 3,)),
            dma((CHUNKS,)),
            dma((CHUNKS,)),
            dma((CHUNKS * NX,)),
            dma((CHUNKS * NX,)),
            dma((CHUNKS * 3,)),
            dma((CHUNKS * 3,)),
            dma((CHUNKS * 3,)),
            dma((CHUNKS * 3,)),
            dma((CHUNKS * 7,)),
            dma((CHUNKS * 7,)),
            dma((14,)),
            dma((14,)),
        ],
        compiler_params=pltpu.CompilerParams(
            collective_id=0, has_side_effects=True, vmem_limit_bytes=50 * 1024 * 1024
        ),
        name="step",
    )(context, target, small, stale)


def update_kernel(
    summed,
    fresh,
    sums,
    weight,
    aggregate,
    moment,
    second,
    aggregate_out,
    weight_out,
    moment_out,
    second_out,
    stale_out,
    norms_out,
    rows_buf,
    norms_buf,
    sem,
):
    copies = [pltpu.make_async_copy(fresh, stale_out, sem.at[0])]
    copies[0].start()
    total = aggregate[...] + summed[...]
    first = 0.9 * moment[...] + 0.1 * total
    scaled = 0.999 * second[...] + 0.001 * total * total
    old = weight[...]
    rows_buf[0] = total
    rows_buf[1] = old - 0.001 * (first / (jnp.sqrt(scaled) + 1e-08) + 0.05 * old)
    rows_buf[2] = first
    rows_buf[3] = scaled
    for i in range(16):
        norms_buf[i] = sums[0, i]
    for i, out in enumerate((aggregate_out, weight_out, moment_out, second_out)):
        copies.append(pltpu.make_async_copy(rows_buf.at[i], out, sem.at[1 + i]))
    copies.append(pltpu.make_async_copy(norms_buf, norms_out, sem.at[5]))
    for copy in copies[1:]:
        copy.start()
    for copy in copies:
        copy.wait()


def update(summed, fresh, sums, weight, aggregate, moment, second):
    vmem = pl.BlockSpec(memory_space=pltpu.VMEM)
    hbm = pl.BlockSpec(memory_space=pltpu.HBM)
    smem = pl.BlockSpec(memory_space=pltpu.SMEM)
    rows = jax.ShapeDtypeStruct(summed.shape, F32)
    return pl.pallas_call(
        update_kernel,
        out_shape=(rows,) * 4
        + (jax.ShapeDtypeStruct(fresh.shape, BF16), jax.ShapeDtypeStruct((16,), F32)),
        in_specs=[vmem, vmem, smem] + [vmem] * 4,
        out_specs=(hbm,) * 6,
        scratch_shapes=[
            pltpu.VMEM((4, *summed.shape), F32),
            pltpu.SMEM((16,), F32),
            pltpu.SemaphoreType.DMA((6,)),
        ],
        compiler_params=pltpu.CompilerParams(vmem_limit_bytes=16 * 1024 * 1024),
        name="update",
    )(summed, fresh, sums, weight, aggregate, moment, second)


def body(context, target, weight, stale, trigger, aggregate, moment, second):
    above, width = weight.shape
    marks = jnp.pad(trigger, ((above, 0), (0, width - trigger.shape[1]))).astype(F32)
    at = lax.broadcasted_iota(jnp.int32, marks.shape, 0)
    small = jnp.where(at < above, jnp.pad(weight, ((0, 1), (0, 0))), marks)
    summed, fresh, sums = step(context, target, small, stale)
    return update(summed, fresh, sums, weight, aggregate, moment, second)


def solution(mesh):
    split = P(("dp", "sub"), None)
    return jax.shard_map(
        body,
        mesh=mesh,
        in_specs=(split, split, split, P(("dp", "sub"), None, None), split, split, split, split),
        out_specs=(split, split, split, split, P(("dp", "sub"), None, None), P()),
        check_vma=False,
    )
```

```python
import functools

import jax
import jax.numpy as jnp
from jax import lax
from jax.experimental import pallas as pl
from jax.experimental.pallas import tpu as pltpu
from jax.sharding import PartitionSpec as P

MESH = pl.DeviceIdType.MESH
F32 = jnp.float32
BF16 = jnp.bfloat16
CHUNKS = 4
NX = 4
NY = 4
NZ = 8
FAR4 = (2, 1, 3)
FAR8 = (4, 3, 5, 2, 6, 1, 7)
PIECE = 4


def step_kernel(
    rows,
    padded,
    context,
    target,
    small,
    stale,
    summed_out,
    stale_out,
    norms_out,
    cbuf,
    ct,
    tbuf,
    sbuf,
    fbuf,
    perm,
    perm_t,
    wz,
    wz32,
    wbuf,
    own_low,
    ebuf,
    half,
    drecv,
    asend,
    arecv,
    bsend,
    brecv,
    zsend,
    zrecv,
    sqacc,
    flags,
    nrm,
    nx_buf,
    ny_buf,
    nz_buf,
    cin_sem,
    tin_sem,
    sin_sem,
    gz_s,
    gz_r,
    gb_s,
    gb_r,
    ge_s,
    ge_r,
    ga_s,
    ga_r,
    gd_s,
    gd_r,
    rd_s,
    rd_r,
    ra_s,
    ra_r,
    rb_s,
    rb_r,
    rz_s,
    rz_r,
    n_s,
    n_r,
):
    width = context.shape[1]
    cols = width // CHUNKS
    dp = lax.axis_index("dp")
    sub = lax.axis_index("sub")
    c = lax.rem(dp, 2)
    x = lax.div(dp, 8)
    zlo = lax.rem(lax.div(dp, 2), 4)
    zhi = lax.div(sub, NY)
    y = lax.rem(sub, NY)
    z = zhi * 4 + zlo
    am = x * (1 - c) + y * c
    bm = y * (1 - c) + x * c

    def device(px, py, pz, pc):
        return ((px * 4 + lax.rem(pz, 4)) * 2 + pc, lax.div(pz, 4) * NY + py)

    def a_peer(a):
        return device(a * (1 - c) + x * c, y * (1 - c) + a * c, z, c)

    def b_peer(b):
        return device(x * (1 - c) + b * c, b * (1 - c) + y * c, z, c)

    def x_peer(k):
        return device(lax.rem(x + k, NX), y, z, c)

    def y_peer(k):
        return device(x, lax.rem(y + k, NY), z, c)

    def z_peer(k):
        return device(x, y, lax.rem(z + k, NZ), c)

    partner = device(x, y, z, 1 - c)

    def remote(src, dst, s, r, to):
        return pltpu.make_async_remote_copy(
            src_ref=src, dst_ref=dst, send_sem=s, recv_sem=r, device_id=to, device_id_type=MESH
        )

    barrier = pltpu.get_barrier_semaphore()
    greeted = [z_peer(k) for k in FAR8]
    greeted += [x_peer(k) for k in FAR4]
    greeted += [y_peer(k) for k in FAR4]
    greeted += [partner]
    for to in greeted:
        pl.semaphore_signal(barrier, inc=1, device_id=to, device_id_type=MESH)

    context_in = pltpu.make_async_copy(context, cbuf.at[pl.ds(0, rows)], cin_sem)
    context_in.start()
    target_in = []
    stale_in = []
    for j in range(CHUNKS):
        part = pl.ds(j * cols, cols)
        target_in.append(
            pltpu.make_async_copy(target.at[:, part], tbuf.at[j, pl.ds(0, rows)], tin_sem.at[j])
        )
        stale_in.append(pltpu.make_async_copy(stale.at[0, :, part], sbuf.at[j], sin_sem.at[j]))
        target_in[j].start()
        stale_in[j].start()

    own_low[...] = small[:PIECE].astype(BF16)
    pl.semaphore_wait(barrier, len(greeted))

    gz = []
    for h in range(2):
        at = pl.ds(h * (width // 2), width // 2)
        for k in FAR8:
            i = h * 7 + k - 1
            gz.append(
                remote(own_low.at[:, at], wz.at[z, :, at], gz_s.at[i], gz_r.at[i], z_peer(k))
            )
            gz[-1].start()
    wz[z] = own_low[...]

    group = 2 * NY * NZ * PIECE
    place = lax.broadcasted_iota(jnp.int32, (group, group), 0)
    natural = lax.broadcasted_iota(jnp.int32, (group, group), 1)

    def natural_of(i):
        ic, iy, iz, ir = i // 128, (i // 32) % 4, (i // 4) % 8, i % 4
        return (iz % 4) * 64 + ic * 32 + (iz // 4) * 16 + iy * 4 + ir

    perm[...] = jnp.where(natural == natural_of(place), 1.0, 0.0).astype(BF16)
    perm_t[...] = jnp.where(place == natural_of(natural), 1.0, 0.0).astype(BF16)
    tail = padded - rows
    cbuf[pl.ds(rows, tail)] = jnp.zeros((tail, width), BF16)
    ebuf[...] = jnp.zeros((padded, cols), BF16)
    for j in range(CHUNKS):
        tbuf[j, pl.ds(rows, tail)] = jnp.zeros((tail, cols), BF16)
    sqacc[...] = jnp.zeros(sqacc.shape, F32)

    context_in.wait()

    def turn(m, carry):
        span = pl.ds(pl.multiple_of(m * 128, 128), 128)
        for g in range(NX):
            at = pl.ds(g * group, group)
            moved = jnp.dot(cbuf[span, at], perm_t[...], preferred_element_type=F32).astype(BF16)
            cbuf[span, at] = moved
            ct[at, span] = moved.T
        return carry

    lax.fori_loop(0, padded // 128, turn, 0)
    gb = []
    for h in range(2):
        for copy in gz[h * 7 : (h + 1) * 7]:
            copy.wait_recv()
        at = pl.ds(h * (width // 2), width // 2)
        for i in range(NZ):
            wz32[pl.ds(i * PIECE, PIECE), at] = wz[i, :, at].astype(F32)
        for j in range(h * 2, h * 2 + 2):
            wbuf[j, c, am, 0] = wz32[:, j * cols : (j + 1) * cols].astype(BF16)
        for j in range(h * 2, h * 2 + 2):
            row = []
            for k in FAR4:
                i = j * 3 + k - 1
                row.append(
                    remote(
                        wbuf.at[j, c, am, 0],
                        wbuf.at[j, c, am, 4 - k],
                        gb_s.at[i],
                        gb_r.at[i],
                        b_peer(lax.rem(bm + k, 4)),
                    )
                )
                row[-1].start()
            gb.append(row)
    ge = []
    for k in FAR4:
        at = wbuf.at[:, c, am, 0]
        ge.append(remote(at, at, ge_s.at[k - 1], ge_r.at[k - 1], a_peer(lax.rem(am + k, 4))))
        ge[-1].start()
    ga = []
    for j in range(CHUNKS):
        for copy in gb[j]:
            copy.wait_recv()
        row = []
        for k in range(1, 4):
            at = wbuf.at[j, c, am, pl.ds(1, 3)]
            i = j * 3 + k - 1
            row.append(remote(at, at, ga_s.at[i], ga_r.at[i], a_peer(lax.rem(am + k, 4))))
            row[-1].start()
        ga.append(row)
    for j in range(CHUNKS):
        stale_in[j].wait()
        for g in range(NX):
            at = pl.ds(g * group, group)
            sbuf[j, at] = jnp.dot(perm[...], sbuf[j, at], preferred_element_type=F32).astype(BF16)
    low = lax.broadcasted_iota(jnp.int32, (16, cols), 0) // PIECE
    marks = small[PIECE : PIECE + 1, :128]
    mark_at = lax.broadcasted_iota(jnp.int32, (1, 128), 1)
    for g in range(NX):
        flag = jnp.zeros((16, cols), F32)
        for i in range(4):
            one = jnp.sum(
                jnp.where(mark_at == g * 4 + i, marks, 0.0), axis=1, keepdims=True
            )
            flag = jnp.where(low == i, one, flag)
        flags[g] = flag

    gd = []

    def to_partner(j):
        for copy in ga[j]:
            copy.wait_recv()
        at = wbuf.at[j, c]
        gd.append(remote(at, at, gd_s.at[j], gd_r.at[j], partner))
        gd[-1].start()

    scale = 1.0 / rows
    tile = -(-rows // 48) * 16

    def forward(j):
        parts = []
        for g in range(NX):
            parts += [wbuf[j, 0, g, lax.rem(b - y + 4, 4)] for b in range(4)]
            parts += [wbuf[j, 1, b, lax.rem(g - x + 4, 4)] for b in range(4)]
        low_part = jnp.concatenate(parts, axis=0)
        for m in range(3):
            at = pl.ds(m * tile, tile)
            out = jnp.dot(cbuf[at, :], low_part, preferred_element_type=F32)
            ebuf[at, :] = (out - tbuf[j, at].astype(F32)).astype(BF16)

    def backward(j, first, last):
        for g in range(first, last):
            at = pl.ds(g * group, group)
            grad = jnp.dot(ct[at, :], ebuf[...], preferred_element_type=F32) * scale
            mine = grad.reshape(16, 16, cols)
            past = sbuf[j, at].astype(F32).reshape(16, 16, cols)
            flag = flags[g][None]
            diff = mine - past
            sq = (diff * diff).sum(axis=0)
            sqacc[g] = sqacc[g] + sq[:, : cols // 2] + sq[:, cols // 2 :]
            chosen = (diff * flag).reshape(group, cols).astype(BF16)
            fresh = flag * mine + (1.0 - flag) * past
            fbuf[j, at] = fresh.reshape(group, cols).astype(BF16)
            for b in range(4):
                half[j, 0, g, b] = chosen[b * 32 : (b + 1) * 32]
                half[j, 1, g, b] = chosen[128 + b * 32 : 128 + (b + 1) * 32]

    def finish(j):
        for g in range(NX):
            at = pl.ds(g * group, group)
            stale_out[0, at, pl.ds(j * cols, cols)] = jnp.dot(
                perm_t[...], fbuf[j, at], preferred_element_type=F32
            ).astype(BF16)

    rd, ra, rb, rz = [], [], [], []

    def send_d(j, first, last):
        for g in range(first, last):
            rd.append(
                remote(
                    half.at[j, 1 - c, g],
                    drecv.at[j, g],
                    rd_s.at[j * NX + g],
                    rd_r.at[j * NX + g],
                    partner,
                )
            )
            rd[-1].start()

    def send_a(j):
        for g in range(NX):
            rd[j * NX + g].wait_recv()
            for b in range(4):
                both = half[j, c, g, b].astype(F32) + drecv[j, g, b].astype(F32)
                asend[j, g * (1 - c) + b * c, b * (1 - c) + g * c] = both.astype(BF16)
        row = []
        for k in FAR4:
            a = lax.rem(am + k, 4)
            i = j * 3 + k - 1
            row.append(
                remote(asend.at[j, a], arecv.at[j, k - 1], ra_s.at[i], ra_r.at[i], a_peer(a))
            )
            row[-1].start()
        ra.append(row)

    def send_b(j):
        for copy in ra[j]:
            copy.wait_recv()
        total = asend[j, am].astype(F32)
        for k in range(3):
            total = total + arecv[j, k].astype(F32)
        bsend[j] = total.astype(BF16)
        row = []
        for k in FAR4:
            b = lax.rem(bm + k, 4)
            i = j * 3 + k - 1
            row.append(
                remote(bsend.at[j, b], brecv.at[j, k - 1], rb_s.at[i], rb_r.at[i], b_peer(b))
            )
            row[-1].start()
        rb.append(row)

    def send_z(j):
        for copy in rb[j]:
            copy.wait_recv()
        total = bsend[j, bm].astype(F32)
        for k in range(3):
            total = total + brecv[j, k].astype(F32)
        for i in range(NZ):
            zsend[j, i] = total[i * PIECE : (i + 1) * PIECE].astype(BF16)
        row = []
        for k in FAR8:
            i = j * 7 + k - 1
            row.append(
                remote(
                    zsend.at[j, lax.rem(z + k, NZ)],
                    zrecv.at[j, k - 1],
                    rz_s.at[i],
                    rz_r.at[i],
                    z_peer(k),
                )
            )
            row[-1].start()
        rz.append(row)

    for copy in ge:
        copy.wait_recv()
    to_partner(0)
    for j in range(CHUNKS):
        gd[j].wait_recv()
        target_in[j].wait()
        forward(j)
        if j + 1 < CHUNKS:
            to_partner(j + 1)
        if j >= 1:
            send_a(j - 1)
        if j >= 3:
            send_b(j - 3)
        if j < CHUNKS - 1:
            backward(j, 0, NX)
            send_d(j, 0, NX)
        else:
            backward(j, 0, 2)
            send_d(j, 0, 2)
            backward(j, 2, NX)
            send_d(j, 2, NX)

    def spread(src, bufs, at, peers, first):
        out = []
        for k, to in enumerate(peers):
            out.append(remote(src, bufs.at[at], n_s.at[first + k], n_r.at[first + k], to))
            out[-1].start()
        return out

    pick = lax.broadcasted_iota(jnp.int32, (16, 64), 1) // PIECE
    pick = jnp.where(pick == lax.broadcasted_iota(jnp.int32, (16, 64), 0), 1.0, 0.0)
    block_sums = jnp.dot(
        pick.astype(F32),
        sqacc[...].reshape(64, 128),
        precision=lax.Precision.HIGHEST,
        preferred_element_type=F32,
    )
    block_sums = jnp.broadcast_to(jnp.sum(block_sums, axis=1, keepdims=True), (16, 128))
    row_at = lax.broadcasted_iota(jnp.int32, (16, 128), 0)
    lane_at = lax.broadcasted_iota(jnp.int32, (16, 128), 1)
    nrm[0] = jnp.sum(jnp.where(row_at == lane_at, block_sums, 0.0), axis=0, keepdims=True)
    sent = spread(nrm.at[0], nrm, 1, [partner], 0)
    send_a(3)
    sent[0].wait_recv()
    nx_buf[x] = nrm[0] + nrm[1]
    sent_x = spread(nx_buf.at[x], nx_buf, x, [x_peer(k) for k in FAR4], 1)
    send_b(1)
    send_z(0)
    finish(0)
    finish(1)
    send_b(2)
    finish(2)
    send_z(1)
    finish(3)
    send_b(3)
    for copy in sent_x:
        copy.wait_recv()
    ny_buf[y] = (nx_buf[0] + nx_buf[1]) + (nx_buf[2] + nx_buf[3])
    sent_y = spread(ny_buf.at[y], ny_buf, y, [y_peer(k) for k in FAR4], 4)
    send_z(2)
    send_z(3)
    for copy in sent_y:
        copy.wait_recv()
    nz_buf[z] = (ny_buf[0] + ny_buf[1]) + (ny_buf[2] + ny_buf[3])
    sent_z = spread(nz_buf.at[z], nz_buf, z, [z_peer(k) for k in FAR8], 7)

    for j in range(CHUNKS):
        for copy in rz[j]:
            copy.wait_recv()
        total = zsend[j, z].astype(F32)
        for k in range(NZ - 1):
            total = total + zrecv[j, k].astype(F32)
        summed_out[:, pl.ds(j * cols, cols)] = total
    for copy in sent_z:
        copy.wait_recv()
    every = nz_buf[0]
    for i in range(1, NZ):
        every = every + nz_buf[i]
    norms_out[...] = every

    for copy in gz + ge + gd + rd + sent + sent_x + sent_y + sent_z:
        copy.wait_send()
    for rows_of in (gb, ga, ra, rb, rz):
        for row in rows_of:
            for copy in row:
                copy.wait_send()


def step(context, target, small, stale):
    rows, width = context.shape
    cols = width // CHUNKS
    padded = -(-rows // 128) * 128
    dma = pltpu.SemaphoreType.DMA
    vmem = pl.BlockSpec(memory_space=pltpu.VMEM)
    hbm = pl.BlockSpec(memory_space=pltpu.HBM)
    return pl.pallas_call(
        functools.partial(step_kernel, rows, padded),
        out_shape=(
            jax.ShapeDtypeStruct((PIECE, width), F32),
            jax.ShapeDtypeStruct((1, width, width), BF16),
            jax.ShapeDtypeStruct((1, 128), F32),
        ),
        in_specs=[hbm, hbm, vmem, hbm],
        out_specs=(vmem, vmem, vmem),
        scratch_shapes=[
            pltpu.VMEM((padded, width), BF16),
            pltpu.VMEM((width, padded), BF16),
            pltpu.VMEM((CHUNKS, padded, cols), BF16),
            pltpu.VMEM((CHUNKS, width, cols), BF16),
            pltpu.VMEM((CHUNKS, width, cols), BF16),
            pltpu.VMEM((256, 256), BF16),
            pltpu.VMEM((256, 256), BF16),
            pltpu.VMEM((NZ, PIECE, width), BF16),
            pltpu.VMEM((NZ * PIECE, width), F32),
            pltpu.VMEM((CHUNKS, 2, 4, 4, 32, cols), BF16),
            pltpu.VMEM((PIECE, width), BF16),
            pltpu.VMEM((padded, cols), BF16),
            pltpu.VMEM((CHUNKS, 2, 4, 4, 32, cols), BF16),
            pltpu.VMEM((CHUNKS, 4, 4, 32, cols), BF16),
            pltpu.VMEM((CHUNKS, 4, 4, 32, cols), BF16),
            pltpu.VMEM((CHUNKS, 3, 4, 32, cols), BF16),
            pltpu.VMEM((CHUNKS, 4, 32, cols), BF16),
            pltpu.VMEM((CHUNKS, 3, 32, cols), BF16),
            pltpu.VMEM((CHUNKS, NZ, PIECE, cols), BF16),
            pltpu.VMEM((CHUNKS, NZ - 1, PIECE, cols), BF16),
            pltpu.VMEM((4, 16, 128), F32),
            pltpu.VMEM((4, 16, cols), F32),
            pltpu.VMEM((2, 1, 128), F32),
            pltpu.VMEM((NX, 1, 128), F32),
            pltpu.VMEM((NY, 1, 128), F32),
            pltpu.VMEM((NZ, 1, 128), F32),
            dma,
            dma((CHUNKS,)),
            dma((CHUNKS,)),
            dma((2 * (NZ - 1),)),
            dma((2 * (NZ - 1),)),
            dma((CHUNKS * 3,)),
            dma((CHUNKS * 3,)),
            dma((3,)),
            dma((3,)),
            dma((CHUNKS * 3,)),
            dma((CHUNKS * 3,)),
            dma((CHUNKS,)),
            dma((CHUNKS,)),
            dma((CHUNKS * NX,)),
            dma((CHUNKS * NX,)),
            dma((CHUNKS * 3,)),
            dma((CHUNKS * 3,)),
            dma((CHUNKS * 3,)),
            dma((CHUNKS * 3,)),
            dma((CHUNKS * 7,)),
            dma((CHUNKS * 7,)),
            dma((14,)),
            dma((14,)),
        ],
        compiler_params=pltpu.CompilerParams(
            collective_id=0, has_side_effects=True, vmem_limit_bytes=50 * 1024 * 1024
        ),
        name="step",
    )(context, target, small, stale)


def update_kernel(
    summed,
    fresh,
    sums,
    weight,
    aggregate,
    moment,
    second,
    aggregate_out,
    weight_out,
    moment_out,
    second_out,
    stale_out,
    norms_out,
    rows_buf,
    sums_buf,
    norms_buf,
    sem,
):
    copies = [pltpu.make_async_copy(fresh, stale_out, sem.at[0])]
    copies[0].start()
    sums_in = pltpu.make_async_copy(sums, sums_buf, sem.at[6])
    sums_in.start()
    total = aggregate[...] + summed[...]
    first = 0.9 * moment[...] + 0.1 * total
    scaled = 0.999 * second[...] + 0.001 * total * total
    old = weight[...]
    rows_buf[0] = total
    rows_buf[1] = old - 0.001 * (first / (jnp.sqrt(scaled) + 1e-08) + 0.05 * old)
    rows_buf[2] = first
    rows_buf[3] = scaled
    for i, out in enumerate((aggregate_out, weight_out, moment_out, second_out)):
        copies.append(pltpu.make_async_copy(rows_buf.at[i], out, sem.at[1 + i]))
        copies[-1].start()
    sums_in.wait()
    for i in range(16):
        norms_buf[i] = sums_buf[0, i]
    copies.append(pltpu.make_async_copy(norms_buf, norms_out, sem.at[5]))
    copies[-1].start()
    for copy in copies:
        copy.wait()


def update(summed, fresh, sums, weight, aggregate, moment, second):
    vmem = pl.BlockSpec(memory_space=pltpu.VMEM)
    hbm = pl.BlockSpec(memory_space=pltpu.HBM)
    rows = jax.ShapeDtypeStruct(summed.shape, F32)
    return pl.pallas_call(
        update_kernel,
        out_shape=(rows,) * 4
        + (jax.ShapeDtypeStruct(fresh.shape, BF16), jax.ShapeDtypeStruct((16,), F32)),
        in_specs=[vmem] * 7,
        out_specs=(hbm,) * 6,
        scratch_shapes=[
            pltpu.VMEM((4, *summed.shape), F32),
            pltpu.SMEM((1, 128), F32),
            pltpu.SMEM((16,), F32),
            pltpu.SemaphoreType.DMA((7,)),
        ],
        compiler_params=pltpu.CompilerParams(vmem_limit_bytes=16 * 1024 * 1024),
        name="update",
    )(summed, fresh, sums, weight, aggregate, moment, second)


def body(context, target, weight, stale, trigger, aggregate, moment, second):
    above, width = weight.shape
    marks = jnp.pad(trigger, ((above, 0), (0, width - trigger.shape[1]))).astype(F32)
    at = lax.broadcasted_iota(jnp.int32, marks.shape, 0)
    small = jnp.where(at < above, jnp.pad(weight, ((0, 1), (0, 0))), marks)
    summed, fresh, sums = step(context, target, small, stale)
    return update(summed, fresh, sums, weight, aggregate, moment, second)


def solution(mesh):
    split = P(("dp", "sub"), None)
    return jax.shard_map(
        body,
        mesh=mesh,
        in_specs=(split, split, split, P(("dp", "sub"), None, None), split, split, split, split),
        out_specs=(split, split, split, split, P(("dp", "sub"), None, None), P()),
        check_vma=False,
    )
```
